256 devices in a mesh: bra: 16 (over z_lo, x), ket: 8 (over y, core), mpo: 2 (over z_hi).
Axes of the slice: x: 4, y: 4, z: 8 (z_hi: 2, z_lo: 4; z = z_hi * 4 + z_lo), core: 2. Of those that a mesh axis runs over, the one named last changes fastest.
Arguments:
- left_env: bfloat16 [4, 3072, 3072], P('mpo', 'bra', 'ket'), may hold values from -6 to 6
- site_tensor: bfloat16 [3072, 4, 3072], P('bra', None, 'ket'), may hold values from -0.0546875 to 0.0546875
- block_values: float32 [12, 4, 4], replicated, may hold values from -3 to 3
- pair_in: int32 [12], replicated, may hold values from 0 to 3
- pair_out: int32 [12], replicated, may hold values from 0 to 3, as said below
Outputs:
- new_env: bfloat16 [4, 3072, 3072], P('mpo', 'bra', 'ket')
The draws below stay inside these ranges and needn't reach their ends.
Inputs may be any that keep to these rules, and one draw needn't show every extreme that they name: `pair_out`: every component number 0 to 3 appears at least once.
All inputs are finite; a program needn't handle non-finite values.
Results may differ from the reference program's by a relative error of at most 0.018.
Values may be sent and summed in bfloat16 or wider, within the bound.
No kernel may reach another device: no remote copies, remote signals or barrier semaphores. Data moves between devices by JAX's collectives and lax.ppermute only.
A program may use at most 64 MiB of HBM per device.

```python
import jax
import jax.numpy as jnp
from jax import lax

D = 3072
PHYS = 4
K = 4
NNZ = 12
N_BRA = 16


def draw_pair_out(key, part):
    first = jax.random.permutation(jax.random.fold_in(key, 11), K).astype(jnp.int32)
    extra = jax.random.randint(jax.random.fold_in(key, 12), (NNZ - K,), 0, K).astype(jnp.int32)
    return jnp.concatenate([first, extra]).astype(jnp.int32)


def touch_ends(result, own_key, smallest, high):
    extent = result.shape
    spot = [jax.random.randint(jax.random.fold_in(own_key, axis), (), 0, extent[axis]) for axis in range(len(extent))]
    result = result.at[tuple(spot)].set(smallest)
    longest = extent.index(max(extent))
    spot[longest] = (spot[longest] + 1) % extent[longest]
    return result.at[tuple(spot)].set(high)


def steps_of(rng, dims, split, smallest, top_value):
    def one(dim, parts):
        steps = jax.random.uniform(jax.random.fold_in(jax.random.fold_in(rng, 6), dim), (parts,), jnp.float32, smallest / len(split), top_value / len(split))
        return jnp.repeat(jnp.exp(steps), dims[dim] // parts).reshape((-1,) + (1,) * (len(dims) - dim - 1))

    factor_of = one(*split[0])
    for cut in split[1:]:
        factor_of = factor_of * one(*cut)
    return factor_of


def bell_draw(rng, extent, width, bound, pieces=(), held_as=jnp.bfloat16):
    entries = width * jax.random.normal(rng, extent, jnp.float32)
    if pieces:
        entries = entries * steps_of(rng, extent, pieces, -0.22, 0.18)
    return jnp.clip(entries, -bound, bound).astype(held_as)


def setup_inputs(seed: int = 0) -> dict:
    streams_of = jax.random.split(jax.random.key(seed), 6)
    left_env = bell_draw(streams_of[0], (K, D, D), 1.0, 6.0, ((0, 2), (1, 16), (2, 8)))
    site_tensor = bell_draw(streams_of[1], (D, PHYS, D), (PHYS * D) ** -0.5, 0.0546875, ((0, 16), (2, 8)))
    block_values = bell_draw(streams_of[2], (NNZ, PHYS, PHYS), 0.5, 3.0, (), jnp.float32)
    pair_in = touch_ends(jax.random.randint(streams_of[3], (NNZ,), 0, K), jax.random.fold_in(streams_of[3], 1), 0, K - 1).astype(jnp.int32)
    pair_out = draw_pair_out(jax.random.fold_in(streams_of[5], 71), 0)
    return {"left_env": left_env, "site_tensor": site_tensor, "block_values": block_values, "pair_in": pair_in, "pair_out": pair_out}


def reference(left_env, site_tensor, block_values, pair_in, pair_out):
    comps = jnp.arange(K, dtype=jnp.int32)
    hot_out = (pair_out[:, None] == comps[None, :]).astype(jnp.float32)
    hot_in = (pair_in[:, None] == comps[None, :]).astype(jnp.float32)
    mixing = jnp.einsum("pv,pw,pst->vswt", hot_out, hot_in, block_values, precision=lax.Precision.HIGHEST)
    flat_site = site_tensor.reshape(D, PHYS * D)

    def one_comp(env):
        return jnp.dot(env, flat_site, preferred_element_type=jnp.float32).astype(jnp.bfloat16)

    half = lax.map(one_comp, left_env).reshape(K, D, PHYS, D)
    mixed = jnp.einsum("vswt,watc->vasc", mixing, half.astype(jnp.float32), precision=lax.Precision.HIGHEST).astype(jnp.bfloat16)
    rows_blk = D // N_BRA

    def add_block(index, total):
        start = (index * rows_blk).astype(jnp.int32)
        site_blk = lax.dynamic_slice_in_dim(site_tensor, start, rows_blk, 0).reshape(rows_blk * PHYS, D)
        mixed_blk = lax.dynamic_slice_in_dim(mixed, start, rows_blk, 1).reshape(K, rows_blk * PHYS, D)
        term = jnp.einsum("ke,wkc->wec", site_blk.astype(jnp.float32), mixed_blk.astype(jnp.float32))
        return total + term.astype(jnp.bfloat16).astype(jnp.float32)

    total = lax.fori_loop(0, N_BRA, add_block, jnp.zeros((K, D, D), jnp.float32))
    return total.astype(jnp.bfloat16)
```

```python
import functools

import jax
import jax.numpy as jnp
from jax import lax
from jax.experimental import pallas as pl
from jax.experimental.pallas import tpu as pltpu
from jax.sharding import Mesh
from jax.sharding import PartitionSpec as P


AXES = ("zl", "x", "y", "core", "zh")
F32, BF16 = jnp.float32, jnp.bfloat16


def _zi(z):
    return (z % 4) * 2 + z // 4


def shift_z(v, k):
    return lax.ppermute(v, ("zl", "zh"), [(_zi(z), _zi((z + k) % 8)) for z in range(8)])


def shift_y(v, k):
    return lax.ppermute(v, "y", [(i, (i + k) % 4) for i in range(4)])


def flip_x(v, j):
    return lax.ppermute(v, "x", [(i, i ^ j) for i in range(4)])


def swap(v):
    return lax.ppermute(v, "core", [(0, 1), (1, 0)])


def call(body, outs, arrays, smem=(), scratch=(), mib=24, flops=0, nbytes=0):
    vm = pl.BlockSpec(memory_space=pltpu.VMEM)
    return pl.pallas_call(
        body,
        out_shape=outs,
        in_specs=[pl.BlockSpec(memory_space=pltpu.SMEM)] * len(smem) + [vm] * len(arrays),
        out_specs=jax.tree.map(lambda _: vm, outs),
        scratch_shapes=list(scratch),
        compiler_params=pltpu.CompilerParams(vmem_limit_bytes=mib * 1024 * 1024),
        cost_estimate=pl.CostEstimate(flops=flops, bytes_accessed=nbytes, transcendentals=0),
    )(*smem, *arrays)


def low_lanes(shape):
    return lax.broadcasted_iota(jnp.int32, shape, 1) < 64


def place():
    return [lax.axis_index(a) for a in AXES]


def prep_body(s_ref, *outs):
    zl, _, _, _, zh = place()

    def write(out, half, lo, hi):
        rows = slice(lo, hi)
        main = slice(0, 128) if half == 0 else slice(256, 384)
        for p in range(2):
            base = p * 384
            out[:, base : base + 128] = s_ref[2 * p, rows, main]
            out[:, base + 128 : base + 256] = s_ref[2 * p + 1, rows, main]
            a = s_ref[2 * p, rows, 128:256].astype(F32)
            b = s_ref[2 * p + 1, rows, 128:256].astype(F32)
            if half == 0:
                b = pltpu.roll(b, 64, 1)
            else:
                a = pltpu.roll(a, 64, 1)
            out[:, base + 256 : base + 384] = jnp.where(low_lanes(a.shape), a, b).astype(BF16)

    for i, out in enumerate(outs):
        lo, hi = ((0, 192), (0, 192), (0, 192), (0, 96), (96, 192))[i]
        dest = ((zh * 4 + zl + (0, 1, 7, 2, 6)[i]) % 8) // 4
        for half in range(2):
            pl.when(dest == half)(functools.partial(write, out, half, lo, hi))


def coef_body(bv, p_in, p_out, coef, mix):
    zh = place()[4]

    def zero(i, _):
        mix[i] = 0.0
        return 0

    lax.fori_loop(0, 256, zero, 0)

    def add(p, _):
        v = p_out[p]
        w = (p_in[p] + 2 * zh) % 4
        for s in range(4):
            for t in range(4):
                i = (v * 4 + s) * 16 + w * 4 + t
                mix[i] = mix[i] + bv[p * 16 + s * 4 + t]
        return 0

    lax.fori_loop(0, 12, add, 0)

    def main(i, _):
        rows = [jnp.full((1, 128), mix[i * 8 + k], F32) for k in range(8)]
        coef[pl.ds(pl.multiple_of(i * 8, 8), 8), :] = jnp.concatenate(rows, axis=0)
        return 0

    lax.fori_loop(0, 32, main, 0)
    low = low_lanes((1, 128))

    def half(i, _):
        rows = []
        for k in range(2):
            g = i * 2 + k
            vp, s, w = g // 16, (g // 4) % 4, g % 4
            for q in range(4):
                lo = mix[(2 * vp * 4 + s) * 16 + w * 4 + (0, 1, 2, 3)[q]]
                hi = mix[((2 * vp + 1) * 4 + s) * 16 + w * 4 + (1, 0, 3, 2)[q]]
                rows.append(jnp.where(low, jnp.full((1, 128), lo, F32), jnp.full((1, 128), hi, F32)))
        coef[pl.ds(pl.multiple_of(256 + i * 8, 8), 8), :] = jnp.concatenate(rows, axis=0)
        return 0

    lax.fori_loop(0, 16, half, 0)


def align_body(mine, other, out):
    zl, x, y, core, _ = place()
    parity, same = x % 2, (x // 2) == core

    def run(par, sm):
        def step(r, _):
            ry = (zl + r - y + 4) % 4
            for j in range(4):
                src = mine if ((j < 2) == sm) else other
                start = ((par + j) % 2) * 192
                out[j, r] = src[ry, :, start : start + 192]
            return 0

        lax.fori_loop(0, 4, step, 0)

    for par in range(2):
        for sm in range(2):
            pl.when((parity == par) & (same == (sm == 1)))(functools.partial(run, par, sm == 1))


def block(s, r, cols):
    own, near, far = s
    if r == 0:
        return own[:, cols]
    if r == 2:
        return far[:, cols]
    return near[r // 2, :, cols]


def products(e, s_of, js, cols):
    total = None
    for j in js:
        for r in range(4):
            d = jnp.dot(e[j, r], block(s_of[j], r, cols), preferred_element_type=F32)
            total = d if total is None else total + d
    return total


def first_body(e, *refs):
    s_of = {j: refs[3 * i : 3 * i + 3] for i, j in enumerate((0, 1, 3))}
    out = refs[9]

    def n_step(n, _):
        cols = pl.ds(pl.multiple_of(n * 256, 256), 256)
        out[:, cols] = products(e, s_of, (0, 1, 3), cols)
        return 0

    lax.fori_loop(0, 3, n_step, 0)


def half_body(coef, part, e0, e1, *refs):
    s_of = {j: refs[3 * i : 3 * i + 3] for i, j in enumerate((0, 1, 3, 2))}
    out, acc = refs[12], refs[13]

    def n_step(n, _):
        cols = pl.ds(pl.multiple_of(n * 256, 256), 256)
        acc[1, :, cols] = products(e1, s_of, (0, 1, 3, 2), cols)
        acc[0, :, cols] = part[:, cols] + products(e0, s_of, (2,), cols)
        return 0

    lax.fori_loop(0, 3, n_step, 0)

    tile_of = (0, 1, 3, 4)
    rows = 16

    def a_step(i, _):
        a0 = pl.multiple_of(i * rows, rows)

        def tile(w, k):
            return acc[w // 2, pl.ds((w % 2) * 192 + a0, rows), k * 128 : (k + 1) * 128]

        for v in range(4):
            lane = (v // 2) * 384 + (v % 2) * 128
            totals = [None] * 4
            for w in range(4):
                for t in range(4):
                    x = tile(w, tile_of[t])
                    for s in range(4):
                        idx = (v * 4 + s) * 16 + w * 4 + t
                        d = coef[idx : idx + 1, :] * x
                        totals[s] = d if totals[s] is None else totals[s] + d
            for s in range(4):
                out[pl.ds(s * 192 + a0, rows), lane : lane + 128] = totals[s].astype(BF16)
        totals = [None] * 8
        for w in range(4):
            for q in range(4):
                x = tile(w, 2 if q < 2 else 5)
                if q % 2:
                    x = pltpu.roll(x, 64, 1)
                for vs in range(8):
                    idx = 256 + vs * 16 + w * 4 + q
                    d = coef[idx : idx + 1, :] * x
                    totals[vs] = d if totals[vs] is None else totals[vs] + d
        for vs in range(8):
            lane = (vs // 4) * 384 + 256
            out[pl.ds((vs % 4) * 192 + a0, rows), lane : lane + 128] = totals[vs].astype(BF16)
        return 0

    lax.fori_loop(0, 192 // rows, a_step, 0)


def term_body(js, quarters, m_ref, mine, other, *outs):
    _, x, y, core, _ = place()
    same = (x // 2) == core

    def run(sm):
        def z_step(zl, _):
            ry = (zl - y + 4) % 4
            for i, j in enumerate(js):
                src = mine if ((j < 2) == sm) else other
                row0 = pl.multiple_of(((x + j) % 2) * 192, 192)
                d = jnp.dot(
                    src[ry, pl.ds(row0, 192), :], m_ref[...], preferred_element_type=F32
                ).astype(BF16)
                if quarters:
                    for q in range(4):
                        outs[4 * i + q][zl] = d[48 * q : 48 * (q + 1)]
                else:
                    outs[i][zl] = d
            return 0

        lax.fori_loop(0, 4, z_step, 0)

    for sm in range(2):
        pl.when(same == (sm == 1))(functools.partial(run, sm == 1))


def zprep_body(c, o0, s1, t3, s3, t1, *outs):
    zl0, _, _, _, zh = place()
    for k in range(8):
        z = (zh * 4 + zl0 + k) % 8
        zl = z % 4
        lane = pl.ds(pl.multiple_of((z // 4) * 384, 128), 384)
        for q, (u, v) in enumerate(((s1, t3), (s3, t1))):
            own = o0[zl, (2 * c + q) * 48 : (2 * c + q + 1) * 48, lane]
            outs[k][48 * q : 48 * (q + 1)] = (
                own.astype(F32) + u[zl, :, lane].astype(F32) + v[zl, :, lane].astype(F32)
            ).astype(BF16)


def final_body(*refs):
    ins, out = refs[:16], refs[16]
    zl0, _, _, _, zh = place()
    for c in range(2):
        rows = slice(c * 96, (c + 1) * 96)
        a0 = jnp.zeros((96, 384), F32)
        a1 = jnp.zeros((96, 384), F32)
        for k in range(8):
            v = ins[8 * c + k][...].astype(F32)
            first = ((zh * 4 + zl0 + 8 - k) % 8) < 4
            a0 = a0 + jnp.where(first, v, 0.0)
            a1 = a1 + jnp.where(first, 0.0, v)
        h0, h1 = a0[:, 256:], a1[:, 256:]
        low = low_lanes(h0.shape)
        out[0, rows, 0:128] = a0[:, 0:128].astype(BF16)
        out[1, rows, 0:128] = a0[:, 128:256].astype(BF16)
        out[0, rows, 128:256] = jnp.where(low, h0, pltpu.roll(h1, 64, 1)).astype(BF16)
        out[1, rows, 128:256] = jnp.where(low, pltpu.roll(h0, 64, 1), h1).astype(BF16)
        out[0, rows, 256:384] = a1[:, 0:128].astype(BF16)
        out[1, rows, 256:384] = a1[:, 128:256].astype(BF16)


def sds(*shape, dtype=BF16):
    return jax.ShapeDtypeStruct(shape, dtype)


ZK = (3, 5, 4, 2, 6, 1, 7)


def add16(a, b):
    return (a.astype(F32) + b.astype(F32)).astype(BF16)


def program(left_env, site_tensor, block_values, pair_in, pair_out):
    env = left_env.reshape(384, 384)
    st = jnp.transpose(site_tensor, (1, 0, 2))
    set_ = jnp.transpose(st.reshape(768, 384))
    ea = shift_y(env, -1)
    eb = shift_y(env, 1)
    ec = shift_y(env, 2)
    a_own, a_p, a_m, a_p2, a_m2 = call(
        prep_body,
        [sds(192, 768), sds(192, 768), sds(192, 768), sds(96, 768), sds(96, 768)],
        [st],
        nbytes=4 << 20,
    )
    za = shift_z(a_m, -1)
    zb = shift_z(a_p, 1)
    zc = shift_z(a_p2, 2)
    zd = shift_z(a_m2, -2)
    xa1 = flip_x(a_own, 1)
    xa3 = flip_x(a_own, 3)
    ez = shift_z(env, 4)
    coef = call(
        coef_body,
        sds(384, 128, dtype=F32),
        [],
        smem=[block_values.reshape(192), pair_in, pair_out],
        scratch=[pltpu.SMEM((256,), F32)],
        nbytes=1 << 20,
    )
    sa = shift_y(set_, -1)
    sb = shift_y(set_, 1)
    near = jnp.stack([za, zb])
    xb1 = flip_x(near, 1)
    xb3 = flip_x(near, 3)
    xf0 = flip_x(xa1, 3)
    far = jnp.concatenate([zc, zd])
    xc1 = flip_x(far, 1)
    xc3 = flip_x(far, 3)
    e_own = jnp.stack([env, ea, ec, eb])
    e_own_s = swap(e_own)
    fa = shift_y(ez, -1)
    fb = shift_y(ez, 1)
    fc = shift_y(ez, 2)
    xf13 = flip_x(xb3, 1)
    xf2 = flip_x(xc1, 3)
    e0 = call(align_body, sds(4, 4, 384, 192), [e_own, e_own_s], nbytes=8 << 20)
    sc = shift_y(sa[:192], -1)
    sd = shift_y(sb[192:], 1)
    s_own, s_1, s_3 = (a_own, near, far), (xa1, xb1, xc1), (xa3, xb3, xc3)
    s_2 = (xf0, xf13, xf2)
    part = call(
        first_body,
        sds(384, 768, dtype=F32),
        [e0, *s_own, *s_1, *s_3],
        flops=2 * 384 * 768 * 2304,
        nbytes=8 << 20,
    )
    e_oth = jnp.stack([ez, fa, fc, fb])
    e_oth_s = swap(e_oth)
    se = jnp.stack([set_, sa, jnp.concatenate([sc, sd]), sb])
    se_s = swap(se)
    e1 = call(align_body, sds(4, 4, 384, 192), [e_oth, e_oth_s], nbytes=8 << 20)
    mixed = call(
        half_body,
        sds(768, 768),
        [coef, part, e0, e1, *s_own, *s_1, *s_3, *s_2],
        scratch=[pltpu.VMEM((2, 384, 768), F32)],
        mib=32,
        flops=2 * 384 * 768 * 3840,
        nbytes=12 << 20,
    )
    qt = sds(4, 48, 768)

    def terms(js, quarters, outs):
        return call(
            functools.partial(term_body, js, quarters),
            outs,
            [mixed, se, se_s],
            flops=2 * 768 * 768 * 768 * len(js),
            nbytes=(4 << 20) * len(js),
        )

    o2 = terms((2,), True, [qt] * 4)
    r1, r3 = [None] * 2, [None] * 2
    for c in range(2):
        r1[c] = flip_x(o2[2 * c], 1)
        r3[c] = flip_x(o2[2 * c + 1], 3)
    o13 = terms((1, 3), True, [qt] * 8)
    o1, o3 = o13[:4], o13[4:]
    s1, s3, t3, t1 = [None] * 2, [None] * 2, [None] * 2, [None] * 2
    for c in range(2):
        s1[c] = flip_x(o1[2 * c], 1)
        s3[c] = flip_x(o3[2 * c + 1], 3)
        t3[c] = flip_x(add16(o3[2 * c], r1[c]), 3)
        t1[c] = flip_x(add16(o1[2 * c + 1], r3[c]), 1)
    (o0,) = terms((0,), False, [sds(4, 192, 768)])
    got = []
    for c in range(2):
        blk = call(
            functools.partial(zprep_body, c),
            [sds(96, 384)] * 8,
            [o0, s1[c], t3[c], s3[c], t1[c]],
            nbytes=4 << 20,
        )
        sent = {k: shift_z(blk[k], k) for k in ZK}
        got += [blk[0]] + [sent[k] for k in range(1, 8)]
    return call(final_body, sds(2, 192, 384), got, nbytes=2 << 20)


def solution(mesh):
    finer = Mesh(mesh.devices.reshape(4, 4, 4, 2, 2), AXES)
    return jax.shard_map(
        program,
        mesh=finer,
        in_specs=(P("zh", ("zl", "x"), ("y", "core")), P(("zl", "x"), None, ("y", "core")), P(), P(), P()),
        out_specs=P("zh", ("zl", "x"), ("y", "core")),
        check_vma=False,
    )
```

```python
import functools

import jax
import jax.numpy as jnp
from jax import lax
from jax.experimental import pallas as pl
from jax.experimental.pallas import tpu as pltpu
from jax.sharding import Mesh
from jax.sharding import PartitionSpec as P


AXES = ("zl", "x", "y", "core", "zh")
F32, BF16 = jnp.float32, jnp.bfloat16


def _zi(z):
    return (z % 4) * 2 + z // 4


def shift_z(v, k):
    return lax.ppermute(v, ("zl", "zh"), [(_zi(z), _zi((z + k) % 8)) for z in range(8)])


def shift_y(v, k):
    return lax.ppermute(v, "y", [(i, (i + k) % 4) for i in range(4)])


def flip_x(v, j):
    return lax.ppermute(v, "x", [(i, i ^ j) for i in range(4)])


def flip_z(v, j):
    return lax.ppermute(v, "zl", [(i, i ^ j) for i in range(4)])


def swap(v):
    return lax.ppermute(v, "core", [(0, 1), (1, 0)])


def call(body, outs, arrays, smem=(), scratch=(), mib=12, flops=0, nbytes=0):
    vm = pl.BlockSpec(memory_space=pltpu.VMEM)
    return pl.pallas_call(
        body,
        out_shape=outs,
        in_specs=[pl.BlockSpec(memory_space=pltpu.SMEM)] * len(smem) + [vm] * len(arrays),
        out_specs=jax.tree.map(lambda _: vm, outs),
        scratch_shapes=list(scratch),
        compiler_params=pltpu.CompilerParams(vmem_limit_bytes=mib * 1024 * 1024),
        cost_estimate=pl.CostEstimate(flops=flops, bytes_accessed=nbytes, transcendentals=0),
    )(*smem, *arrays)


def low_lanes(shape):
    return lax.broadcasted_iota(jnp.int32, shape, 1) < 64


def place():
    return [lax.axis_index(a) for a in AXES]


def prep_body(s_ref, _, *refs):
    outs, both = refs[:5], refs[5]
    zl, _, _, _, zh = place()

    def step(p, _):
        base = pl.multiple_of(p * 384, 384)

        def put(half, at, v):
            both[half, :, pl.ds(base + at, 128)] = v

        s0, s1 = s_ref.at[2 * p], s_ref.at[2 * p + 1]
        for half in range(2):
            main = slice(half * 256, half * 256 + 128)
            put(half, 0, s0[:, main])
            put(half, 128, s1[:, main])
        a, b = s0[:, 128:256].astype(F32), s1[:, 128:256].astype(F32)
        low = low_lanes(a.shape)
        put(0, 256, jnp.where(low, a, pltpu.roll(b, 64, 1)).astype(BF16))
        put(1, 256, jnp.where(low, pltpu.roll(a, 64, 1), b).astype(BF16))
        return 0

    lax.fori_loop(0, 2, step, 0)
    for i, out in enumerate(outs):
        lo, hi = ((0, 192), (0, 192), (0, 192), (0, 96), (96, 192))[i]
        dest = ((zh * 4 + zl + (0, 1, 7, 2, 6)[i]) % 8) // 4
        out[...] = both[dest, lo:hi]


def coef_body(bv, p_in, p_out, coef, mix):
    zh = place()[4]

    def zero(i, _):
        mix[i] = 0.0
        return 0

    lax.fori_loop(0, 256, zero, 0)

    def add(p, _):
        v = p_out[p]
        w = (p_in[p] + 2 * zh) % 4
        for s in range(4):
            for t in range(4):
                i = (v * 4 + s) * 16 + w * 4 + t
                mix[i] = mix[i] + bv[s, t, p]
        return 0

    lax.fori_loop(0, 12, add, 0)

    def main(i, _):
        rows = [jnp.full((1, 128), mix[i * 8 + k], F32) for k in range(8)]
        coef[pl.ds(pl.multiple_of(i * 8, 8), 8), :] = jnp.concatenate(rows, axis=0)
        return 0

    lax.fori_loop(0, 32, main, 0)
    low = low_lanes((1, 128))

    def half(i, _):
        rows = []
        for k in range(2):
            g = i * 2 + k
            vp, s, w = g // 16, (g // 4) % 4, g % 4
            for q in range(4):
                lo = mix[(2 * vp * 4 + s) * 16 + w * 4 + (0, 1, 2, 3)[q]]
                hi = mix[((2 * vp + 1) * 4 + s) * 16 + w * 4 + (1, 0, 3, 2)[q]]
                rows.append(jnp.where(low, jnp.full((1, 128), lo, F32), jnp.full((1, 128), hi, F32)))
        coef[pl.ds(pl.multiple_of(256 + i * 8, 8), 8), :] = jnp.concatenate(rows, axis=0)
        return 0

    lax.fori_loop(0, 16, half, 0)


def copy_body(*refs):
    out = refs[-1]
    for i, ref in enumerate(refs[:-1]):
        out[i] = ref[...]


def align_body(mine, other, out):
    zl, x, y, core, _ = place()
    parity, same = x % 2, (x // 2) == core

    def run(par, sm):
        def step(n, _):
            r = n // 4
            ry = (zl + r - y + 4) % 4
            part = pl.ds(pl.multiple_of((n % 4) * 96, 96), 96)
            for j in range(4):
                src = mine if ((j < 2) == sm) else other
                start = ((par + j) % 2) * 192
                out[j, r, part] = src[ry, part, start : start + 192]
            return 0

        lax.fori_loop(0, 16, step, 0)

    for par in range(2):
        for sm in range(2):
            pl.when((parity == par) & (same == (sm == 1)))(functools.partial(run, par, sm == 1))


def block(s, r, cols):
    own, near, far = s
    if r == 0:
        return own[:, cols]
    if r == 2:
        return far[:, cols]
    return near[r // 2, :, cols]


def products(e, s_of, js, cols):
    total = None
    for j in js:
        for r in range(4):
            d = jnp.dot(e[j, r], block(s_of[j], r, cols), preferred_element_type=F32)
            total = d if total is None else total + d
    return total


def inputs(refs):
    return {j: refs[3 * i : 3 * i + 3] for i, j in enumerate((0, 1, 3))}


def first_body(e, *refs):
    s_of, out = inputs(refs), refs[9]

    def n_step(n, _):
        cols = pl.ds(pl.multiple_of(n * 256, 256), 256)
        out[:, cols] = products(e, s_of, (0, 1, 3), cols)
        return 0

    lax.fori_loop(0, 3, n_step, 0)


def half_body(coef, part, e0, e1, *refs):
    s_of = inputs(refs)
    s_of[2] = (refs[9].at[0], refs[10], refs[9].at[1])
    out, acc = refs[11], refs[12]

    def n_step(n, _):
        cols = pl.ds(pl.multiple_of(n * 256, 256), 256)
        acc[1, :, cols] = products(e1, s_of, (0, 1, 3, 2), cols)
        acc[0, :, cols] = part[:, cols] + products(e0, s_of, (2,), cols)
        return 0

    lax.fori_loop(0, 3, n_step, 0)

    tile_of = (0, 1, 3, 4)
    rows = 16

    def a_step(i, _):
        a0 = pl.multiple_of(i * rows, rows)

        def tile(w, k):
            return acc[w // 2, pl.ds((w % 2) * 192 + a0, rows), k * 128 : (k + 1) * 128]

        for v in range(4):
            lane = (v // 2) * 384 + (v % 2) * 128
            totals = [None] * 4
            for w in range(4):
                for t in range(4):
                    x = tile(w, tile_of[t])
                    for s in range(4):
                        idx = (v * 4 + s) * 16 + w * 4 + t
                        d = coef[idx : idx + 1, :] * x
                        totals[s] = d if totals[s] is None else totals[s] + d
            for s in range(4):
                out[pl.ds(s * 192 + a0, rows), lane : lane + 128] = totals[s].astype(BF16)
        totals = [None] * 8
        for w in range(4):
            for q in range(4):
                x = tile(w, 2 if q < 2 else 5)
                if q % 2:
                    x = pltpu.roll(x, 64, 1)
                for vs in range(8):
                    idx = 256 + vs * 16 + w * 4 + q
                    d = coef[idx : idx + 1, :] * x
                    totals[vs] = d if totals[vs] is None else totals[vs] + d
        for vs in range(8):
            lane = (vs // 4) * 384 + 256
            out[pl.ds((vs % 4) * 192 + a0, rows), lane : lane + 128] = totals[vs].astype(BF16)
        return 0

    lax.fori_loop(0, 192 // rows, a_step, 0)


def terms_of(js, rows, m_ref, mine, other, write):
    _, x, y, core, _ = place()
    same = (x // 2) == core

    def run(sm):
        def step(zl, _):
            ry = (zl - y + 4) % 4
            for j in js:
                src = mine if ((j < 2) == sm) else other
                lo, hi = rows(j)
                row0 = pl.multiple_of(((x + j) % 2) * 192 + lo, 96)
                d = jnp.dot(
                    src[ry, pl.ds(row0, hi - lo), :], m_ref[...], preferred_element_type=F32
                ).astype(BF16)
                write(j, zl, d)
            return 0

        lax.fori_loop(0, 4, step, 0)

    for sm in range(2):
        pl.when(same == (sm == 1))(functools.partial(run, sm == 1))


def term2_body(m_ref, mine, other, ra, rb):
    def write(j, zl, d):
        ra[zl], rb[zl] = d[:48], d[48:]

    terms_of((2,), lambda j: (0, 96), m_ref, mine, other, write)


def term_body(m_ref, mine, other, m1, m3, s1b, s3b, t1, t3):
    def write(j, zl, d):
        if j == 2:
            m1[1, zl], m3[1, zl] = d[:48], d[48:]
        elif j == 1:
            m1[0, zl], s1b[zl] = d[0:48], d[96:144]
            t1[0, zl], t1[1, zl] = d[48:96], d[144:192]
        else:
            m3[0, zl], s3b[zl] = d[48:96], d[144:192]
            t3[0, zl], t3[1, zl] = d[0:48], d[96:144]

    def rows(j):
        return (96, 192) if j == 2 else (0, 192)

    terms_of((2, 1, 3), rows, m_ref, mine, other, write)


def term0_body(m_ref, mine, other, o0):
    def write(j, zl, d):
        o0[zl] = d

    terms_of((0,), lambda j: (0, 192), m_ref, mine, other, write)


def add_body(a, ra, b, rb, oa, ob):
    oa[...] = (a[0].astype(F32) + ra[...].astype(F32)).astype(BF16)
    ob[...] = (b[0].astype(F32) + rb[...].astype(F32)).astype(BF16)


def add2_body(a, ra, b, rb, oa, ob):
    oa[...] = (a[1].astype(F32) + ra[1].astype(F32)).astype(BF16)
    ob[...] = (b[1].astype(F32) + rb[1].astype(F32)).astype(BF16)


def se_body(s0, s1, c, d, s3, out):
    out[0], out[1], out[3] = s0[...], s1[...], s3[...]
    out[2, :192], out[2, 192:] = c[...], d[...]


def split_body(a, b, oa, ob):
    oa[...], ob[...] = a[:192], b[192:]


def join_body(a, b, out):
    out[:96], out[96:] = a[...], b[...]


def zprep0_body(o0, m1, t3, m3, t1, *outs):
    zl0 = place()[0]
    for k in range(4):
        zl = zl0 ^ k
        for q, (u, v) in enumerate(((m1.at[0], t3), (m3.at[0], t1))):
            own = o0[zl, q * 48 : (q + 1) * 48]
            outs[k][48 * q : 48 * (q + 1)] = (
                own.astype(F32) + u[zl].astype(F32) + v[zl].astype(F32)
            ).astype(BF16)


def zsum_body(a, b, c, d, keep, give):
    zh = place()[4]

    def run(half):
        for h in range(2):
            cols = slice(h * 384, (h + 1) * 384)
            total = a[:, cols].astype(F32)
            for r in (b, c, d):
                total = total + r[:, cols].astype(F32)
            if h == half:
                keep[...] = total
            else:
                give[...] = total.astype(BF16)

    for half in range(2):
        pl.when(zh == half)(functools.partial(run, half))


def zlast_body(o0, s1, t3, s3, t1, *outs):
    zl0, _, _, _, zh = place()
    for k in range(8):
        z = (zh * 4 + zl0 + k) % 8
        zl = z % 4
        lane = pl.ds(pl.multiple_of((z // 4) * 384, 128), 384)
        for q, (u, v) in enumerate(((s1, t3), (s3, t1))):
            own = o0[zl, (2 + q) * 48 : (3 + q) * 48, lane]
            outs[k][48 * q : 48 * (q + 1)] = (
                own.astype(F32) + u[zl, :, lane].astype(F32) + v[zl, :, lane].astype(F32)
            ).astype(BF16)


def final_body(keep, give, *refs):
    ins, out = refs[:8], refs[8]
    zl0, _, _, _, zh = place()
    z0 = zh * 4 + zl0

    def write(row0, i, a0, a1):
        rows = pl.ds(pl.multiple_of(row0 + i * 32, 32), 32)
        h0, h1 = a0[:, 256:], a1[:, 256:]
        low = low_lanes(h0.shape)
        out[0, rows, 0:128] = a0[:, 0:128].astype(BF16)
        out[1, rows, 0:128] = a0[:, 128:256].astype(BF16)
        out[0, rows, 128:256] = jnp.where(low, h0, pltpu.roll(h1, 64, 1)).astype(BF16)
        out[1, rows, 128:256] = jnp.where(low, pltpu.roll(h0, 64, 1), h1).astype(BF16)
        out[0, rows, 256:384] = a1[:, 0:128].astype(BF16)
        out[1, rows, 256:384] = a1[:, 128:256].astype(BF16)

    def step(i, _):
        part = pl.ds(pl.multiple_of(i * 32, 32), 32)
        kept, got = keep[part], give[part].astype(F32)
        first = zh == 0
        write(0, i, jnp.where(first, kept, got), jnp.where(first, got, kept))
        a0 = jnp.zeros((32, 384), F32)
        a1 = jnp.zeros((32, 384), F32)
        for k in range(8):
            v = ins[k][part].astype(F32)
            low_z = ((z0 + 8 - k) % 8) < 4
            a0 = a0 + jnp.where(low_z, v, 0.0)
            a1 = a1 + jnp.where(low_z, 0.0, v)
        write(96, i, a0, a1)
        return 0

    lax.fori_loop(0, 3, step, 0)


def sds(*shape, dtype=BF16):
    return jax.ShapeDtypeStruct(shape, dtype)


def program(left_env, site_tensor, block_values, pair_in, pair_out):
    env = left_env.reshape(384, 384)
    st = jnp.transpose(site_tensor, (1, 0, 2))
    set_ = jnp.transpose(st.reshape(768, 384))
    ea = shift_y(env, -1)
    eb = shift_y(env, 1)
    a_own, a_p, a_m, a_p2, a_m2 = call(
        prep_body,
        [sds(192, 768), sds(192, 768), sds(192, 768), sds(96, 768), sds(96, 768)],
        [st, set_],
        scratch=[pltpu.VMEM((2, 192, 768), BF16)],
        nbytes=4 << 20,
    )
    za = shift_z(a_m, -1)
    zb = shift_z(a_p, 1)
    zc = shift_z(a_p2, 2)
    zd = shift_z(a_m2, -2)
    xa1 = flip_x(a_own, 1)
    xa3 = flip_x(a_own, 3)
    ec = shift_y(env, 2)
    ez = shift_z(env, 4)
    sa = shift_y(set_, -1)
    sb = shift_y(set_, 1)
    near = call(copy_body, sds(2, 192, 768), [za, zb], nbytes=1 << 20)
    xb1 = flip_x(near, 1)
    xb3 = flip_x(near, 3)
    far = call(join_body, sds(192, 768), [zc, zd], nbytes=1 << 20)
    xc1 = flip_x(far, 1)
    xc3 = flip_x(far, 3)
    e_own = call(copy_body, sds(4, 384, 384), [env, ea, ec, eb], nbytes=2 << 20)
    e_own_s = swap(e_own)
    coef = call(
        coef_body,
        sds(384, 128, dtype=F32),
        [],
        smem=[jnp.transpose(block_values, (1, 2, 0)), pair_in, pair_out],
        scratch=[pltpu.SMEM((256,), F32)],
        nbytes=1 << 20,
    )
    fa = shift_y(ez, -1)
    fb = shift_y(ez, 1)
    fc = shift_y(ez, 2)
    e0 = call(align_body, sds(4, 4, 384, 192), [e_own, e_own_s], nbytes=8 << 20)
    sa2, sb2 = call(split_body, [sds(192, 768)] * 2, [sa, sb], nbytes=1 << 20)
    sc = shift_y(sa2, -1)
    sd = shift_y(sb2, 1)
    xf13 = flip_x(xb3, 1)
    pair = call(copy_body, sds(2, 192, 768), [xa1, xc1], nbytes=1 << 20)
    xf02 = flip_x(pair, 3)
    s_in = [a_own, near, far, xa1, xb1, xc1, xa3, xb3, xc3]
    part = call(
        first_body,
        sds(384, 768, dtype=F32),
        [e0, *s_in],
        flops=2 * 384 * 768 * 2304,
        nbytes=8 << 20,
    )
    e_oth = call(copy_body, sds(4, 384, 384), [ez, fa, fc, fb], nbytes=2 << 20)
    e_oth_s = swap(e_oth)
    e1 = call(align_body, sds(4, 4, 384, 192), [e_oth, e_oth_s], nbytes=8 << 20)
    se = call(se_body, sds(4, 384, 768), [set_, sa, sc, sd, sb], nbytes=6 << 20)
    se_s = swap(se)
    mixed = call(
        half_body,
        sds(768, 768),
        [coef, part, e0, e1, *s_in, xf02, xf13],
        scratch=[pltpu.VMEM((2, 384, 768), F32)],
        mib=20,
        flops=2 * 384 * 768 * 3840,
        nbytes=12 << 20,
    )
    qt, q2 = sds(4, 48, 768), sds(2, 4, 48, 768)
    args = [mixed, se, se_s]
    ra, rb = call(term2_body, [qt, qt], args, mib=16, flops=1 << 30, nbytes=4 << 20)
    r1 = flip_x(ra, 1)
    r3 = flip_x(rb, 3)
    m1, m3, s1b, s3b, t1q, t3q = call(
        term_body, [q2, q2, qt, qt, q2, q2], args, mib=16, flops=1 << 31, nbytes=8 << 20
    )
    m1 = flip_x(m1, 1)
    m3 = flip_x(m3, 3)
    ta, tb = call(add_body, [qt, qt], [t3q, r1, t1q, r3], nbytes=2 << 20)
    t3, t1 = [None] * 2, [None] * 2
    t3[0] = flip_x(ta, 3)
    t1[0] = flip_x(tb, 1)
    s1b = flip_x(s1b, 1)
    s3b = flip_x(s3b, 3)
    ta, tb = call(add2_body, [qt, qt], [t3q, m1, t1q, m3], nbytes=2 << 20)
    t3[1] = flip_x(ta, 3)
    t1[1] = flip_x(tb, 1)
    (o0,) = call(term0_body, [sds(4, 192, 768)], args, mib=16, flops=1 << 30, nbytes=6 << 20)
    got = call(zprep0_body, [sds(96, 768)] * 4, [o0, m1, t3[0], m3, t1[0]], nbytes=4 << 20)
    got = [got[0]] + [flip_z(got[k], k) for k in (1, 2, 3)]
    last = call(zlast_body, [sds(96, 384)] * 8, [o0, s1b, t3[1], s3b, t1[1]], nbytes=4 << 20)
    last = [last[0]] + [shift_z(last[k], k) for k in range(1, 8)]
    keep, give = call(zsum_body, [sds(96, 384, dtype=F32), sds(96, 384)], got, nbytes=1 << 20)
    give = shift_z(give, 4)
    return call(final_body, sds(2, 192, 384), [keep, give, *last], nbytes=2 << 20)


def solution(mesh):
    finer = Mesh(mesh.devices.reshape(4, 4, 4, 2, 2), AXES)
    return jax.shard_map(
        program,
        mesh=finer,
        in_specs=(P("zh", ("zl", "x"), ("y", "core")), P(("zl", "x"), None, ("y", "core")), P(), P(), P()),
        out_specs=P("zh", ("zl", "x"), ("y", "core")),
        check_vma=False,
    )
```

```python
import functools

import jax
import jax.numpy as jnp
from jax import lax
from jax.experimental import pallas as pl
from jax.experimental.pallas import tpu as pltpu
from jax.sharding import Mesh
from jax.sharding import PartitionSpec as P


AXES = ("zl", "x", "y", "core", "zh")
F32, BF16 = jnp.float32, jnp.bfloat16


def _zi(z):
    return (z % 4) * 2 + z // 4


def shift_z(v, k):
    return lax.ppermute(v, ("zl", "zh"), [(_zi(z), _zi((z + k) % 8)) for z in range(8)])


def shift_y(v, k):
    return lax.ppermute(v, "y", [(i, (i + k) % 4) for i in range(4)])


def flip_x(v, j):
    return lax.ppermute(v, "x", [(i, i ^ j) for i in range(4)])


def flip_z(v, j):
    return lax.ppermute(v, "zl", [(i, i ^ j) for i in range(4)])


def swap(v):
    return lax.ppermute(v, "core", [(0, 1), (1, 0)])


def call(body, outs, arrays, smem=(), scratch=(), mib=12, flops=0, nbytes=0):
    vm = pl.BlockSpec(memory_space=pltpu.VMEM)
    return pl.pallas_call(
        body,
        out_shape=outs,
        in_specs=[pl.BlockSpec(memory_space=pltpu.SMEM)] * len(smem) + [vm] * len(arrays),
        out_specs=jax.tree.map(lambda _: vm, outs),
        scratch_shapes=list(scratch),
        compiler_params=pltpu.CompilerParams(vmem_limit_bytes=mib * 1024 * 1024),
        cost_estimate=pl.CostEstimate(flops=flops, bytes_accessed=nbytes, transcendentals=0),
    )(*smem, *arrays)


def low_lanes(shape):
    return lax.broadcasted_iota(jnp.int32, shape, 1) < 64


def place():
    return [lax.axis_index(a) for a in AXES]


def prep_body(s_ref, _, *refs):
    outs, both = refs[:5], refs[5]
    zl, _, _, _, zh = place()

    def step(p, _):
        base = pl.multiple_of(p * 384, 384)

        def put(half, at, v):
            both[half, :, pl.ds(base + at, 128)] = v

        s0, s1 = s_ref.at[2 * p], s_ref.at[2 * p + 1]
        for half in range(2):
            main = slice(half * 256, half * 256 + 128)
            put(half, 0, s0[:, main])
            put(half, 128, s1[:, main])
        a, b = s0[:, 128:256].astype(F32), s1[:, 128:256].astype(F32)
        low = low_lanes(a.shape)
        put(0, 256, jnp.where(low, a, pltpu.roll(b, 64, 1)).astype(BF16))
        put(1, 256, jnp.where(low, pltpu.roll(a, 64, 1), b).astype(BF16))
        return 0

    lax.fori_loop(0, 2, step, 0)
    for i, out in enumerate(outs):
        lo, hi = ((0, 192), (0, 192), (0, 192), (0, 96), (96, 192))[i]
        dest = ((zh * 4 + zl + (0, 1, 7, 2, 6)[i]) % 8) // 4
        out[...] = both[dest, lo:hi]


def coef_body(bv, p_in, p_out, coef, mix):
    zh = place()[4]

    def zero(i, _):
        mix[i] = 0.0
        return 0

    lax.fori_loop(0, 256, zero, 0)

    def add(p, _):
        v = p_out[p]
        w = (p_in[p] + 2 * zh) % 4
        for s in range(4):
            for t in range(4):
                i = (v * 4 + s) * 16 + w * 4 + t
                mix[i] = mix[i] + bv[s, t, p]
        return 0

    lax.fori_loop(0, 12, add, 0)

    def main(i, _):
        rows = [jnp.full((1, 128), mix[i * 8 + k], F32) for k in range(8)]
        coef[pl.ds(pl.multiple_of(i * 8, 8), 8), :] = jnp.concatenate(rows, axis=0)
        return 0

    lax.fori_loop(0, 32, main, 0)
    low = low_lanes((1, 128))

    def half(i, _):
        rows = []
        for k in range(2):
            g = i * 2 + k
            vp, s, w = g // 16, (g // 4) % 4, g % 4
            for q in range(4):
                lo = mix[(2 * vp * 4 + s) * 16 + w * 4 + (0, 1, 2, 3)[q]]
                hi = mix[((2 * vp + 1) * 4 + s) * 16 + w * 4 + (1, 0, 3, 2)[q]]
                rows.append(jnp.where(low, jnp.full((1, 128), lo, F32), jnp.full((1, 128), hi, F32)))
        coef[pl.ds(pl.multiple_of(256 + i * 8, 8), 8), :] = jnp.concatenate(rows, axis=0)
        return 0

    lax.fori_loop(0, 16, half, 0)


def copy_body(*refs):
    out = refs[-1]
    for i, ref in enumerate(refs[:-1]):
        out[i] = ref[...]


def align_body(mine, other, out):
    zl, x, y, core, _ = place()
    parity, same = x % 2, (x // 2) == core

    def run(par, sm):
        def step(r, _):
            ry = (zl + r - y + 4) % 4
            for j in range(4):
                src = mine if ((j < 2) == sm) else other
                start = ((par + j) % 2) * 192
                out[j, r] = src[ry, :, start : start + 192]
            return 0

        lax.fori_loop(0, 4, step, 0)

    for par in range(2):
        for sm in range(2):
            pl.when((parity == par) & (same == (sm == 1)))(functools.partial(run, par, sm == 1))


def block(s, r, cols):
    own, near, far = s
    if r == 0:
        return own[:, cols]
    if r == 2:
        return far[:, cols]
    return near[r // 2, :, cols]


def products(e, s_of, js, cols):
    total = None
    for j in js:
        for r in range(4):
            d = jnp.dot(e[j, r], block(s_of[j], r, cols), preferred_element_type=F32)
            total = d if total is None else total + d
    return total


def inputs(refs):
    return {j: refs[3 * i : 3 * i + 3] for i, j in enumerate((0, 1, 3))}


def first_body(e, *refs):
    s_of, out = inputs(refs), refs[9]

    def n_step(n, _):
        cols = pl.ds(pl.multiple_of(n * 256, 256), 256)
        out[:, cols] = products(e, s_of, (0, 1, 3), cols)
        return 0

    lax.fori_loop(0, 3, n_step, 0)


def half_body(coef, part, e0, e1, *refs):
    s_of = inputs(refs)
    s_of[2] = (refs[9].at[0], refs[10], refs[9].at[1])
    out, acc = refs[11], refs[12]

    def n_step(n, _):
        cols = pl.ds(pl.multiple_of(n * 256, 256), 256)
        acc[1, :, cols] = products(e1, s_of, (0, 1, 3, 2), cols)
        acc[0, :, cols] = part[:, cols] + products(e0, s_of, (2,), cols)
        return 0

    lax.fori_loop(0, 3, n_step, 0)

    tile_of = (0, 1, 3, 4)
    rows = 16

    def a_step(i, _):
        a0 = pl.multiple_of(i * rows, rows)

        def tile(w, k):
            return acc[w // 2, pl.ds((w % 2) * 192 + a0, rows), k * 128 : (k + 1) * 128]

        for v in range(4):
            lane = (v // 2) * 384 + (v % 2) * 128
            totals = [None] * 4
            for w in range(4):
                for t in range(4):
                    x = tile(w, tile_of[t])
                    for s in range(4):
                        idx = (v * 4 + s) * 16 + w * 4 + t
                        d = coef[idx : idx + 1, :] * x
                        totals[s] = d if totals[s] is None else totals[s] + d
            for s in range(4):
                out[pl.ds(s * 192 + a0, rows), lane : lane + 128] = totals[s].astype(BF16)
        totals = [None] * 8
        for w in range(4):
            for q in range(4):
                x = tile(w, 2 if q < 2 else 5)
                if q % 2:
                    x = pltpu.roll(x, 64, 1)
                for vs in range(8):
                    idx = 256 + vs * 16 + w * 4 + q
                    d = coef[idx : idx + 1, :] * x
                    totals[vs] = d if totals[vs] is None else totals[vs] + d
        for vs in range(8):
            lane = (vs // 4) * 384 + 256
            out[pl.ds((vs % 4) * 192 + a0, rows), lane : lane + 128] = totals[vs].astype(BF16)
        return 0

    lax.fori_loop(0, 192 // rows, a_step, 0)


def terms_of(js, rows, m_ref, mine, other, write):
    _, x, y, core, _ = place()
    same = (x // 2) == core

    def run(sm):
        def step(zl, _):
            ry = (zl - y + 4) % 4
            for j in js:
                src = mine if ((j < 2) == sm) else other
                lo, hi = rows(j)
                row0 = pl.multiple_of(((x + j) % 2) * 192 + lo, 96)
                d = jnp.dot(
                    src[ry, pl.ds(row0, hi - lo), :], m_ref[...], preferred_element_type=F32
                ).astype(BF16)
                write(j, zl, d)
            return 0

        lax.fori_loop(0, 4, step, 0)

    for sm in range(2):
        pl.when(same == (sm == 1))(functools.partial(run, sm == 1))


def term2_body(m_ref, mine, other, ra, rb):
    def write(j, zl, d):
        ra[zl], rb[zl] = d[:48], d[48:]

    terms_of((2,), lambda j: (0, 96), m_ref, mine, other, write)


def term_body(m_ref, mine, other, m1, m3, s1b, s3b, t1, t3):
    def write(j, zl, d):
        if j == 2:
            m1[1, zl], m3[1, zl] = d[:48], d[48:]
        elif j == 1:
            m1[0, zl], s1b[zl] = d[0:48], d[96:144]
            t1[0, zl], t1[1, zl] = d[48:96], d[144:192]
        else:
            m3[0, zl], s3b[zl] = d[48:96], d[144:192]
            t3[0, zl], t3[1, zl] = d[0:48], d[96:144]

    def rows(j):
        return (96, 192) if j == 2 else (0, 192)

    terms_of((2, 1, 3), rows, m_ref, mine, other, write)


def term0_body(m_ref, mine, other, o0):
    def write(j, zl, d):
        o0[zl] = d

    terms_of((0,), lambda j: (0, 192), m_ref, mine, other, write)


def add_body(a, ra, b, rb, oa, ob):
    oa[...] = (a[0].astype(F32) + ra[...].astype(F32)).astype(BF16)
    ob[...] = (b[0].astype(F32) + rb[...].astype(F32)).astype(BF16)


def add2_body(a, ra, b, rb, oa, ob):
    oa[...] = (a[1].astype(F32) + ra[1].astype(F32)).astype(BF16)
    ob[...] = (b[1].astype(F32) + rb[1].astype(F32)).astype(BF16)


def se_body(s0, s1, c, d, s3, out):
    out[0], out[1], out[3] = s0[...], s1[...], s3[...]
    out[2, :192], out[2, 192:] = c[...], d[...]


def split_body(a, b, oa, ob):
    oa[...], ob[...] = a[:192], b[192:]


def join_body(a, b, out):
    out[:96], out[96:] = a[...], b[...]


def zprep0_body(o0, m1, t3, m3, t1, own, far, pair):
    zl0 = place()[0]
    for k, out in enumerate((own, pair.at[0], far, pair.at[1])):
        zl = zl0 ^ k
        for q, (u, v) in enumerate(((m1.at[0], t3), (m3.at[0], t1))):
            o = o0[zl, q * 48 : (q + 1) * 48]
            out[48 * q : 48 * (q + 1)] = (
                o.astype(F32) + u[zl].astype(F32) + v[zl].astype(F32)
            ).astype(BF16)


def zmid_body(own, far, pair, a, b):
    a[...] = own[...].astype(F32) + pair[0].astype(F32)
    b[...] = (far[...].astype(F32) + pair[1].astype(F32)).astype(BF16)


def zsum_body(a, b, keep, give):
    zh = place()[4]

    def run(half):
        for h in range(2):
            cols = slice(h * 384, (h + 1) * 384)
            total = a[:, cols] + b[:, cols].astype(F32)
            if h == half:
                keep[...] = total
            else:
                give[...] = total.astype(BF16)

    for half in range(2):
        pl.when(zh == half)(functools.partial(run, half))


def zlast_body(o0, s1, t3, s3, t1, *outs):
    zl0, _, _, _, zh = place()
    for k in range(8):
        z = (zh * 4 + zl0 + k) % 8
        zl = z % 4
        lane = pl.ds(pl.multiple_of((z // 4) * 384, 128), 384)
        for q, (u, v) in enumerate(((s1, t3), (s3, t1))):
            own = o0[zl, (2 + q) * 48 : (3 + q) * 48, lane]
            outs[k][48 * q : 48 * (q + 1)] = (
                own.astype(F32) + u[zl, :, lane].astype(F32) + v[zl, :, lane].astype(F32)
            ).astype(BF16)


def final_body(keep, give, *refs):
    ins, out = refs[:8], refs[8]
    zl0, _, _, _, zh = place()
    z0 = zh * 4 + zl0

    def write(row0, i, a0, a1):
        rows = pl.ds(pl.multiple_of(row0 + i * 32, 32), 32)
        h0, h1 = a0[:, 256:], a1[:, 256:]
        low = low_lanes(h0.shape)
        out[0, rows, 0:128] = a0[:, 0:128].astype(BF16)
        out[1, rows, 0:128] = a0[:, 128:256].astype(BF16)
        out[0, rows, 128:256] = jnp.where(low, h0, pltpu.roll(h1, 64, 1)).astype(BF16)
        out[1, rows, 128:256] = jnp.where(low, pltpu.roll(h0, 64, 1), h1).astype(BF16)
        out[0, rows, 256:384] = a1[:, 0:128].astype(BF16)
        out[1, rows, 256:384] = a1[:, 128:256].astype(BF16)

    def step(i, _):
        part = pl.ds(pl.multiple_of(i * 32, 32), 32)
        kept, got = keep[part], give[part].astype(F32)
        first = zh == 0
        write(0, i, jnp.where(first, kept, got), jnp.where(first, got, kept))
        a0 = jnp.zeros((32, 384), F32)
        a1 = jnp.zeros((32, 384), F32)
        for k in range(8):
            v = ins[k][part].astype(F32)
            low_z = ((z0 + 8 - k) % 8) < 4
            a0 = a0 + jnp.where(low_z, v, 0.0)
            a1 = a1 + jnp.where(low_z, 0.0, v)
        write(96, i, a0, a1)
        return 0

    lax.fori_loop(0, 3, step, 0)


def sds(*shape, dtype=BF16):
    return jax.ShapeDtypeStruct(shape, dtype)


def program(left_env, site_tensor, block_values, pair_in, pair_out):
    env = left_env.reshape(384, 384)
    st = jnp.transpose(site_tensor, (1, 0, 2))
    set_ = jnp.transpose(st.reshape(768, 384))
    ea = shift_y(env, -1)
    eb = shift_y(env, 1)
    a_own, a_p, a_m, a_p2, a_m2 = call(
        prep_body,
        [sds(192, 768), sds(192, 768), sds(192, 768), sds(96, 768), sds(96, 768)],
        [st, set_],
        scratch=[pltpu.VMEM((2, 192, 768), BF16)],
        nbytes=4 << 20,
    )
    za = shift_z(a_m, -1)
    zb = shift_z(a_p, 1)
    zc = shift_z(a_p2, 2)
    zd = shift_z(a_m2, -2)
    xa1 = flip_x(a_own, 1)
    xa3 = flip_x(a_own, 3)
    ec = shift_y(env, 2)
    ez = shift_z(env, 4)
    sa = shift_y(set_, -1)
    sb = shift_y(set_, 1)
    near = call(copy_body, sds(2, 192, 768), [za, zb], nbytes=1 << 20)
    xb1 = flip_x(near, 1)
    xb3 = flip_x(near, 3)
    far = call(join_body, sds(192, 768), [zc, zd], nbytes=1 << 20)
    xc1 = flip_x(far, 1)
    xc3 = flip_x(far, 3)
    e_own = call(copy_body, sds(4, 384, 384), [env, ea, ec, eb], nbytes=2 << 20)
    e_own_s = swap(e_own)
    coef = call(
        coef_body,
        sds(384, 128, dtype=F32),
        [],
        smem=[jnp.transpose(block_values, (1, 2, 0)), pair_in, pair_out],
        scratch=[pltpu.SMEM((256,), F32)],
        nbytes=1 << 20,
    )
    fa = shift_y(ez, -1)
    fb = shift_y(ez, 1)
    fc = shift_y(ez, 2)
    e0 = call(align_body, sds(4, 4, 384, 192), [e_own, e_own_s], nbytes=8 << 20)
    sa2, sb2 = call(split_body, [sds(192, 768)] * 2, [sa, sb], nbytes=1 << 20)
    sc = shift_y(sa2, -1)
    sd = shift_y(sb2, 1)
    xf13 = flip_x(xb3, 1)
    pair = call(copy_body, sds(2, 192, 768), [xa1, xc1], nbytes=1 << 20)
    xf02 = flip_x(pair, 3)
    s_in = [a_own, near, far, xa1, xb1, xc1, xa3, xb3, xc3]
    part = call(
        first_body,
        sds(384, 768, dtype=F32),
        [e0, *s_in],
        flops=2 * 384 * 768 * 2304,
        nbytes=8 << 20,
    )
    e_oth = call(copy_body, sds(4, 384, 384), [ez, fa, fc, fb], nbytes=2 << 20)
    e_oth_s = swap(e_oth)
    e1 = call(align_body, sds(4, 4, 384, 192), [e_oth, e_oth_s], nbytes=8 << 20)
    se = call(se_body, sds(4, 384, 768), [set_, sa, sc, sd, sb], nbytes=6 << 20)
    se_s = swap(se)
    mixed = call(
        half_body,
        sds(768, 768),
        [coef, part, e0, e1, *s_in, xf02, xf13],
        scratch=[pltpu.VMEM((2, 384, 768), F32)],
        mib=20,
        flops=2 * 384 * 768 * 3840,
        nbytes=12 << 20,
    )
    qt, q2 = sds(4, 48, 768), sds(2, 4, 48, 768)
    args = [mixed, se, se_s]
    ra, rb = call(term2_body, [qt, qt], args, mib=16, flops=1 << 30, nbytes=4 << 20)
    r1 = flip_x(ra, 1)
    r3 = flip_x(rb, 3)
    m1, m3, s1b, s3b, t1q, t3q = call(
        term_body, [q2, q2, qt, qt, q2, q2], args, mib=16, flops=1 << 31, nbytes=8 << 20
    )
    m1 = flip_x(m1, 1)
    m3 = flip_x(m3, 3)
    ta, tb = call(add_body, [qt, qt], [t3q, r1, t1q, r3], nbytes=2 << 20)
    t3, t1 = [None] * 2, [None] * 2
    t3[0] = flip_x(ta, 3)
    t1[0] = flip_x(tb, 1)
    s1b = flip_x(s1b, 1)
    s3b = flip_x(s3b, 3)
    ta, tb = call(add2_body, [qt, qt], [t3q, m1, t1q, m3], nbytes=2 << 20)
    t3[1] = flip_x(ta, 3)
    t1[1] = flip_x(tb, 1)
    (o0,) = call(term0_body, [sds(4, 192, 768)], args, mib=16, flops=1 << 30, nbytes=6 << 20)
    own, fard, pairs = call(
        zprep0_body,
        [sds(96, 768), sds(96, 768), sds(2, 96, 768)],
        [o0, m1, t3[0], m3, t1[0]],
        nbytes=4 << 20,
    )
    pairs = flip_z(pairs, 1)
    a, b = call(
        zmid_body, [sds(96, 768, dtype=F32), sds(96, 768)], [own, fard, pairs], nbytes=1 << 20
    )
    b = flip_z(b, 2)
    last = call(zlast_body, [sds(96, 384)] * 8, [o0, s1b, t3[1], s3b, t1[1]], nbytes=4 << 20)
    last = [last[0]] + [shift_z(last[k], k) for k in range(1, 8)]
    keep, give = call(zsum_body, [sds(96, 384, dtype=F32), sds(96, 384)], [a, b], nbytes=1 << 20)
    give = shift_z(give, 4)
    return call(final_body, sds(2, 192, 384), [keep, give, *last], nbytes=2 << 20)


def solution(mesh):
    finer = Mesh(mesh.devices.reshape(4, 4, 4, 2, 2), AXES)
    return jax.shard_map(
        program,
        mesh=finer,
        in_specs=(P("zh", ("zl", "x"), ("y", "core")), P(("zl", "x"), None, ("y", "core")), P(), P(), P()),
        out_specs=P("zh", ("zl", "x"), ("y", "core")),
        check_vma=False,
    )
```

```python
import functools

import jax
import jax.numpy as jnp
from jax import lax
from jax.experimental import pallas as pl
from jax.experimental.pallas import tpu as pltpu
from jax.sharding import Mesh
from jax.sharding import PartitionSpec as P


AXES = ("zl", "x", "y", "core", "zh")
F32, BF16 = jnp.float32, jnp.bfloat16


def _zi(z):
    return (z % 4) * 2 + z // 4


def shift_z(v, k):
    return lax.ppermute(v, ("zl", "zh"), [(_zi(z), _zi((z + k) % 8)) for z in range(8)])


def shift_y(v, k):
    return lax.ppermute(v, "y", [(i, (i + k) % 4) for i in range(4)])


def flip_x(v, j):
    return lax.ppermute(v, "x", [(i, i ^ j) for i in range(4)])


def flip_z(v, j):
    return lax.ppermute(v, "zl", [(i, i ^ j) for i in range(4)])


def swap(v):
    return lax.ppermute(v, "core", [(0, 1), (1, 0)])


def call(body, outs, arrays, smem=(), scratch=(), mib=12, flops=0, nbytes=0):
    vm = pl.BlockSpec(memory_space=pltpu.VMEM)
    return pl.pallas_call(
        body,
        out_shape=outs,
        in_specs=[pl.BlockSpec(memory_space=pltpu.SMEM)] * len(smem) + [vm] * len(arrays),
        out_specs=jax.tree.map(lambda _: vm, outs),
        scratch_shapes=list(scratch),
        compiler_params=pltpu.CompilerParams(vmem_limit_bytes=mib * 1024 * 1024),
        cost_estimate=pl.CostEstimate(flops=flops, bytes_accessed=nbytes, transcendentals=0),
    )(*smem, *arrays)


def low_lanes(shape):
    return lax.broadcasted_iota(jnp.int32, shape, 1) < 64


def place():
    return [lax.axis_index(a) for a in AXES]


def prep_body(s_ref, _, *refs):
    outs, both = refs[:5], refs[5]
    zl, _, _, _, zh = place()

    def step(p, _):
        base = pl.multiple_of(p * 384, 384)

        def put(half, at, v):
            both[half, :, pl.ds(base + at, 128)] = v

        s0, s1 = s_ref.at[2 * p], s_ref.at[2 * p + 1]
        for half in range(2):
            main = slice(half * 256, half * 256 + 128)
            put(half, 0, s0[:, main])
            put(half, 128, s1[:, main])
        a, b = s0[:, 128:256].astype(F32), s1[:, 128:256].astype(F32)
        low = low_lanes(a.shape)
        put(0, 256, jnp.where(low, a, pltpu.roll(b, 64, 1)).astype(BF16))
        put(1, 256, jnp.where(low, pltpu.roll(a, 64, 1), b).astype(BF16))
        return 0

    lax.fori_loop(0, 2, step, 0)
    for i, out in enumerate(outs):
        lo, hi = ((0, 192), (0, 192), (0, 192), (0, 96), (96, 192))[i]
        dest = ((zh * 4 + zl + (0, 1, 7, 2, 6)[i]) % 8) // 4
        out[...] = both[dest, lo:hi]


def coef_body(bv, p_in, p_out, coef, mix):
    zh = place()[4]

    def zero(i, _):
        mix[i] = 0.0
        return 0

    lax.fori_loop(0, 256, zero, 0)

    def add(p, _):
        v = p_out[p]
        w = (p_in[p] + 2 * zh) % 4
        for s in range(4):
            for t in range(4):
                i = (v * 4 + s) * 16 + w * 4 + t
                mix[i] = mix[i] + bv[s, t, p]
        return 0

    lax.fori_loop(0, 12, add, 0)

    def main(i, _):
        rows = [jnp.full((1, 128), mix[i * 8 + k], F32) for k in range(8)]
        coef[pl.ds(pl.multiple_of(i * 8, 8), 8), :] = jnp.concatenate(rows, axis=0)
        return 0

    lax.fori_loop(0, 32, main, 0)
    low = low_lanes((1, 128))

    def half(i, _):
        rows = []
        for k in range(2):
            g = i * 2 + k
            vp, s, w = g // 16, (g // 4) % 4, g % 4
            for q in range(4):
                lo = mix[(2 * vp * 4 + s) * 16 + w * 4 + (0, 1, 2, 3)[q]]
                hi = mix[((2 * vp + 1) * 4 + s) * 16 + w * 4 + (1, 0, 3, 2)[q]]
                rows.append(jnp.where(low, jnp.full((1, 128), lo, F32), jnp.full((1, 128), hi, F32)))
        coef[pl.ds(pl.multiple_of(256 + i * 8, 8), 8), :] = jnp.concatenate(rows, axis=0)
        return 0

    lax.fori_loop(0, 16, half, 0)


def copy_body(*refs):
    out = refs[-1]
    for i, ref in enumerate(refs[:-1]):
        out[i] = ref[...]


def align_body(mine, other, out):
    zl, x, y, core, _ = place()
    parity, same = x % 2, (x // 2) == core

    def run(par, sm):
        def step(r, _):
            ry = (zl + r - y + 4) % 4
            for j in range(4):
                src = mine if ((j < 2) == sm) else other
                start = ((par + j) % 2) * 192
                out[j, r] = src[ry, :, start : start + 192]
            return 0

        lax.fori_loop(0, 4, step, 0)

    for par in range(2):
        for sm in range(2):
            pl.when((parity == par) & (same == (sm == 1)))(functools.partial(run, par, sm == 1))


def block(s, r, cols):
    own, near, far = s
    if r == 0:
        return own[:, cols]
    if r == 2:
        return far[:, cols]
    return near[r // 2, :, cols]


def products(e, s_of, js, cols):
    total = None
    for j in js:
        for r in range(4):
            d = jnp.dot(e[j, r], block(s_of[j], r, cols), preferred_element_type=F32)
            total = d if total is None else total + d
    return total


def inputs(refs):
    return {j: refs[3 * i : 3 * i + 3] for i, j in enumerate((0, 1, 3))}


def first_body(e, *refs):
    s_of, out = inputs(refs), refs[9]

    def n_step(n, _):
        cols = pl.ds(pl.multiple_of(n * 256, 256), 256)
        out[:, cols] = products(e, s_of, (0, 1, 3), cols)
        return 0

    lax.fori_loop(0, 3, n_step, 0)


def mix_pair(coef, g, acc, before, out):
    tile_of = (0, 1, 3, 4)
    rows = 16

    def a_step(i, _):
        a0 = pl.multiple_of(i * rows, rows)

        def tile(w, k):
            return acc[pl.ds(w * 192 + a0, rows), k * 128 : (k + 1) * 128]

        def put(s, lane, total):
            part = pl.ds(s * 192 + a0, rows)
            if before is not None:
                total = total + before[part, lane : lane + 128]
            out[part, lane : lane + 128] = total.astype(out.dtype)

        for v in range(4):
            totals = [None] * 4
            for w in range(2):
                for t in range(4):
                    x = tile(w, tile_of[t])
                    for s in range(4):
                        idx = (v * 4 + s) * 16 + (2 * g + w) * 4 + t
                        d = coef[idx : idx + 1, :] * x
                        totals[s] = d if totals[s] is None else totals[s] + d
            for s in range(4):
                put(s, (v // 2) * 384 + (v % 2) * 128, totals[s])
        totals = [None] * 8
        for w in range(2):
            for q in range(4):
                x = tile(w, 2 if q < 2 else 5)
                if q % 2:
                    x = pltpu.roll(x, 64, 1)
                for vs in range(8):
                    idx = 256 + vs * 16 + (2 * g + w) * 4 + q
                    d = coef[idx : idx + 1, :] * x
                    totals[vs] = d if totals[vs] is None else totals[vs] + d
        for vs in range(8):
            put(vs % 4, (vs // 4) * 384 + 256, totals[vs])
        return 0

    lax.fori_loop(0, 192 // rows, a_step, 0)


def mid_body(coef, part, e0, pair, near, out, acc):
    def n_step(n, _):
        cols = pl.ds(pl.multiple_of(n * 256, 256), 256)
        acc[:, cols] = part[:, cols] + products(e0, {2: (pair.at[0], near, pair.at[1])}, (2,), cols)
        return 0

    lax.fori_loop(0, 3, n_step, 0)
    mix_pair(coef, 0, acc, None, out)


def half_body(coef, mown, e1, *refs):
    s_of = inputs(refs)
    s_of[2] = (refs[9].at[0], refs[10], refs[9].at[1])
    out, acc = refs[11], refs[12]

    def n_step(n, _):
        cols = pl.ds(pl.multiple_of(n * 256, 256), 256)
        acc[:, cols] = products(e1, s_of, (0, 1, 3, 2), cols)
        return 0

    lax.fori_loop(0, 3, n_step, 0)
    mix_pair(coef, 1, acc, mown, out)


def terms_of(js, rows, m_ref, mine, other, write):
    _, x, y, core, _ = place()
    same = (x // 2) == core

    def run(sm):
        def step(zl, _):
            ry = (zl - y + 4) % 4
            for j in js:
                src = mine if ((j < 2) == sm) else other
                lo, hi = rows(j)
                row0 = pl.multiple_of(((x + j) % 2) * 192 + lo, 96)
                d = jnp.dot(
                    src[ry, pl.ds(row0, hi - lo), :], m_ref[...], preferred_element_type=F32
                ).astype(BF16)
                write(j, zl, d)
            return 0

        lax.fori_loop(0, 4, step, 0)

    for sm in range(2):
        pl.when(same == (sm == 1))(functools.partial(run, sm == 1))


def term2_body(m_ref, mine, other, ra, rb):
    def write(j, zl, d):
        ra[zl], rb[zl] = d[:48], d[48:]

    terms_of((2,), lambda j: (0, 96), m_ref, mine, other, write)


def term_body(m_ref, mine, other, m1, m3, s1b, s3b, t1, t3):
    def write(j, zl, d):
        if j == 2:
            m1[1, zl], m3[1, zl] = d[:48], d[48:]
        elif j == 1:
            m1[0, zl], s1b[zl] = d[0:48], d[96:144]
            t1[0, zl], t1[1, zl] = d[48:96], d[144:192]
        else:
            m3[0, zl], s3b[zl] = d[48:96], d[144:192]
            t3[0, zl], t3[1, zl] = d[0:48], d[96:144]

    def rows(j):
        return (96, 192) if j == 2 else (0, 192)

    terms_of((2, 1, 3), rows, m_ref, mine, other, write)


def term0_body(m_ref, mine, other, o0):
    def write(j, zl, d):
        o0[zl] = d

    terms_of((0,), lambda j: (0, 192), m_ref, mine, other, write)


def add_body(a, ra, b, rb, oa, ob):
    oa[...] = (a[0].astype(F32) + ra[...].astype(F32)).astype(BF16)
    ob[...] = (b[0].astype(F32) + rb[...].astype(F32)).astype(BF16)


def add2_body(a, ra, b, rb, oa, ob):
    oa[...] = (a[1].astype(F32) + ra[1].astype(F32)).astype(BF16)
    ob[...] = (b[1].astype(F32) + rb[1].astype(F32)).astype(BF16)


def se_body(s0, s1, c, d, s3, out):
    out[0], out[1], out[3] = s0[...], s1[...], s3[...]
    out[2, :192], out[2, 192:] = c[...], d[...]


def split_body(a, b, oa, ob):
    oa[...], ob[...] = a[:192], b[192:]


def join_body(a, b, out):
    out[:96], out[96:] = a[...], b[...]


def zprep0_body(o0, m1, t3, m3, t1, own, far, pair):
    zl0 = place()[0]
    for k, out in enumerate((own, pair.at[0], far, pair.at[1])):
        zl = zl0 ^ k
        for q, (u, v) in enumerate(((m1.at[0], t3), (m3.at[0], t1))):
            o = o0[zl, q * 48 : (q + 1) * 48]
            out[48 * q : 48 * (q + 1)] = (
                o.astype(F32) + u[zl].astype(F32) + v[zl].astype(F32)
            ).astype(BF16)


def zmid_body(own, far, pair, a, b):
    a[...] = own[...].astype(F32) + pair[0].astype(F32)
    b[...] = (far[...].astype(F32) + pair[1].astype(F32)).astype(BF16)


def zsum_body(a, b, keep, give):
    zh = place()[4]

    def run(half):
        for h in range(2):
            cols = slice(h * 384, (h + 1) * 384)
            total = a[:, cols] + b[:, cols].astype(F32)
            if h == half:
                keep[...] = total
            else:
                give[...] = total.astype(BF16)

    for half in range(2):
        pl.when(zh == half)(functools.partial(run, half))


def zlast_body(o0, s1, t3, s3, t1, *outs):
    zl0, _, _, _, zh = place()
    for k in range(8):
        z = (zh * 4 + zl0 + k) % 8
        zl = z % 4
        lane = pl.ds(pl.multiple_of((z // 4) * 384, 128), 384)
        for q, (u, v) in enumerate(((s1, t3), (s3, t1))):
            own = o0[zl, (2 + q) * 48 : (3 + q) * 48, lane]
            outs[k][48 * q : 48 * (q + 1)] = (
                own.astype(F32) + u[zl, :, lane].astype(F32) + v[zl, :, lane].astype(F32)
            ).astype(BF16)


def final_body(keep, give, *refs):
    ins, out = refs[:8], refs[8]
    zl0, _, _, _, zh = place()
    z0 = zh * 4 + zl0

    def write(row0, i, a0, a1):
        rows = pl.ds(pl.multiple_of(row0 + i * 32, 32), 32)
        h0, h1 = a0[:, 256:], a1[:, 256:]
        low = low_lanes(h0.shape)
        out[0, rows, 0:128] = a0[:, 0:128].astype(BF16)
        out[1, rows, 0:128] = a0[:, 128:256].astype(BF16)
        out[0, rows, 128:256] = jnp.where(low, h0, pltpu.roll(h1, 64, 1)).astype(BF16)
        out[1, rows, 128:256] = jnp.where(low, pltpu.roll(h0, 64, 1), h1).astype(BF16)
        out[0, rows, 256:384] = a1[:, 0:128].astype(BF16)
        out[1, rows, 256:384] = a1[:, 128:256].astype(BF16)

    def step(i, _):
        part = pl.ds(pl.multiple_of(i * 32, 32), 32)
        kept, got = keep[part], give[part].astype(F32)
        first = zh == 0
        write(0, i, jnp.where(first, kept, got), jnp.where(first, got, kept))
        a0 = jnp.zeros((32, 384), F32)
        a1 = jnp.zeros((32, 384), F32)
        for k in range(8):
            v = ins[k][part].astype(F32)
            low_z = ((z0 + 8 - k) % 8) < 4
            a0 = a0 + jnp.where(low_z, v, 0.0)
            a1 = a1 + jnp.where(low_z, 0.0, v)
        write(96, i, a0, a1)
        return 0

    lax.fori_loop(0, 3, step, 0)


def sds(*shape, dtype=BF16):
    return jax.ShapeDtypeStruct(shape, dtype)


def program(left_env, site_tensor, block_values, pair_in, pair_out):
    env = left_env.reshape(384, 384)
    st = jnp.transpose(site_tensor, (1, 0, 2))
    set_ = jnp.transpose(st.reshape(768, 384))
    ea = shift_y(env, -1)
    eb = shift_y(env, 1)
    a_own, a_p, a_m, a_p2, a_m2 = call(
        prep_body,
        [sds(192, 768), sds(192, 768), sds(192, 768), sds(96, 768), sds(96, 768)],
        [st, set_],
        scratch=[pltpu.VMEM((2, 192, 768), BF16)],
        nbytes=4 << 20,
    )
    za = shift_z(a_m, -1)
    zb = shift_z(a_p, 1)
    zc = shift_z(a_p2, 2)
    zd = shift_z(a_m2, -2)
    xa1 = flip_x(a_own, 1)
    xa3 = flip_x(a_own, 3)
    ec = shift_y(env, 2)
    ez = shift_z(env, 4)
    sa = shift_y(set_, -1)
    sb = shift_y(set_, 1)
    near = call(copy_body, sds(2, 192, 768), [za, zb], nbytes=1 << 20)
    xb1 = flip_x(near, 1)
    xb3 = flip_x(near, 3)
    far = call(join_body, sds(192, 768), [zc, zd], nbytes=1 << 20)
    xc1 = flip_x(far, 1)
    xc3 = flip_x(far, 3)
    e_own = call(copy_body, sds(4, 384, 384), [env, ea, ec, eb], nbytes=2 << 20)
    e_own_s = swap(e_own)
    coef = call(
        coef_body,
        sds(384, 128, dtype=F32),
        [],
        smem=[jnp.transpose(block_values, (1, 2, 0)), pair_in, pair_out],
        scratch=[pltpu.SMEM((256,), F32)],
        nbytes=1 << 20,
    )
    fa = shift_y(ez, -1)
    fb = shift_y(ez, 1)
    fc = shift_y(ez, 2)
    e0 = call(align_body, sds(4, 4, 384, 192), [e_own, e_own_s], nbytes=8 << 20)
    sa2, sb2 = call(split_body, [sds(192, 768)] * 2, [sa, sb], nbytes=1 << 20)
    sc = shift_y(sa2, -1)
    sd = shift_y(sb2, 1)
    xf13 = flip_x(xb3, 1)
    pair = call(copy_body, sds(2, 192, 768), [xa1, xc1], nbytes=1 << 20)
    xf02 = flip_x(pair, 3)
    s_in = [a_own, near, far, xa1, xb1, xc1, xa3, xb3, xc3]
    part = call(
        first_body,
        sds(384, 768, dtype=F32),
        [e0, *s_in],
        flops=2 * 384 * 768 * 2304,
        nbytes=8 << 20,
    )
    e_oth = call(copy_body, sds(4, 384, 384), [ez, fa, fc, fb], nbytes=2 << 20)
    e_oth_s = swap(e_oth)
    e1 = call(align_body, sds(4, 4, 384, 192), [e_oth, e_oth_s], nbytes=8 << 20)
    se = call(se_body, sds(4, 384, 768), [set_, sa, sc, sd, sb], nbytes=6 << 20)
    se_s = swap(se)
    acc = [pltpu.VMEM((384, 768), F32)]
    s_2 = [xf02, xf13]
    mown = call(
        mid_body,
        sds(768, 768, dtype=F32),
        [coef, part, e0, *s_2],
        scratch=acc,
        flops=2 * 384 * 768 * 768,
        nbytes=6 << 20,
    )
    mixed = call(
        half_body,
        sds(768, 768),
        [coef, mown, e1, *s_in, *s_2],
        scratch=acc,
        mib=20,
        flops=2 * 384 * 768 * 3072,
        nbytes=12 << 20,
    )
    qt, q2 = sds(4, 48, 768), sds(2, 4, 48, 768)
    args = [mixed, se, se_s]
    ra, rb = call(term2_body, [qt, qt], args, mib=16, flops=1 << 30, nbytes=4 << 20)
    r1 = flip_x(ra, 1)
    r3 = flip_x(rb, 3)
    m1, m3, s1b, s3b, t1q, t3q = call(
        term_body, [q2, q2, qt, qt, q2, q2], args, mib=16, flops=1 << 31, nbytes=8 << 20
    )
    m1 = flip_x(m1, 1)
    m3 = flip_x(m3, 3)
    ta, tb = call(add_body, [qt, qt], [t3q, r1, t1q, r3], nbytes=2 << 20)
    t3, t1 = [None] * 2, [None] * 2
    t3[0] = flip_x(ta, 3)
    t1[0] = flip_x(tb, 1)
    s1b = flip_x(s1b, 1)
    s3b = flip_x(s3b, 3)
    ta, tb = call(add2_body, [qt, qt], [t3q, m1, t1q, m3], nbytes=2 << 20)
    t3[1] = flip_x(ta, 3)
    t1[1] = flip_x(tb, 1)
    (o0,) = call(term0_body, [sds(4, 192, 768)], args, mib=16, flops=1 << 30, nbytes=6 << 20)
    own, fard, pairs = call(
        zprep0_body,
        [sds(96, 768), sds(96, 768), sds(2, 96, 768)],
        [o0, m1, t3[0], m3, t1[0]],
        nbytes=4 << 20,
    )
    pairs = flip_z(pairs, 1)
    a, b = call(
        zmid_body, [sds(96, 768, dtype=F32), sds(96, 768)], [own, fard, pairs], nbytes=1 << 20
    )
    b = flip_z(b, 2)
    last = call(zlast_body, [sds(96, 384)] * 8, [o0, s1b, t3[1], s3b, t1[1]], nbytes=4 << 20)
    last = [last[0]] + [shift_z(last[k], k) for k in range(1, 8)]
    keep, give = call(zsum_body, [sds(96, 384, dtype=F32), sds(96, 384)], [a, b], nbytes=1 << 20)
    give = shift_z(give, 4)
    return call(final_body, sds(2, 192, 384), [keep, give, *last], nbytes=2 << 20)


def solution(mesh):
    finer = Mesh(mesh.devices.reshape(4, 4, 4, 2, 2), AXES)
    return jax.shard_map(
        program,
        mesh=finer,
        in_specs=(P("zh", ("zl", "x"), ("y", "core")), P(("zl", "x"), None, ("y", "core")), P(), P(), P()),
        out_specs=P("zh", ("zl", "x"), ("y", "core")),
        check_vma=False,
    )
```
